64 devices in a mesh: rep: 4 (over x, y), dp: 16 (over z, core).
Axes of the slice: x: 2, y: 2, z: 8, core: 2. Of those that a mesh axis runs over, the one named last changes fastest.
The devices are a block of a 4x4x8 slice.
Arguments:
- x: bfloat16 [64, 2048, 896], P(('rep', 'dp')), parts along dimension 0
- dy: bfloat16 [64, 2048, 896], P(('rep', 'dp')), parts along dimension 0
- w_gate: bfloat16 [2, 896, 2304], replicated
- w_up: bfloat16 [2, 896, 2304], replicated
- w_down: bfloat16 [2, 2304, 896], replicated
- m_w_gate: float32 [2, 896, 2304], P(None, 'dp')
- m_w_up: float32 [2, 896, 2304], P(None, 'dp')
- m_w_down: float32 [2, 2304, 896], P(None, 'dp')
- v_w_gate: float32 [2, 896, 2304], P(None, 'dp')
- v_w_up: float32 [2, 896, 2304], P(None, 'dp')
- v_w_down: float32 [2, 2304, 896], P(None, 'dp')
Outputs:
- output 1: bfloat16 [8, 896, 2304], P('rep'), parts along dimension 0
- output 2: bfloat16 [8, 896, 2304], P('rep'), parts along dimension 0
- output 3: bfloat16 [8, 2304, 896], P('rep'), parts along dimension 0
- output 4: float32 [8, 896, 2304], P('rep', 'dp'), parts along dimension 0
- output 5: float32 [8, 896, 2304], P('rep', 'dp'), parts along dimension 0
- output 6: float32 [8, 2304, 896], P('rep', 'dp'), parts along dimension 0
- output 7: float32 [8, 896, 2304], P('rep', 'dp'), parts along dimension 0
- output 8: float32 [8, 896, 2304], P('rep', 'dp'), parts along dimension 0
- output 9: float32 [8, 2304, 896], P('rep', 'dp'), parts along dimension 0
There are 4 independent parts. The reference program is written for one: setup_inputs(seed, part) draws one part's arguments, and reference() takes and returns one part's arrays. A program takes and returns all parts, laid end to end along the dimension named above; an argument that names none is the same for every part.
All inputs are finite; a program needn't handle non-finite values.
Results may differ from the reference program's by a relative error of at most 0.022.
Values are sent between devices in bfloat16 or wider.
A program may use at most 768 MiB of HBM per device.

```python
import jax
import jax.numpy as jnp
from jax import lax

SEQUENCES = 16
TOKENS = 2048
D = 896
FF = 2304
LAYERS = 2
NAMES = ("w_gate", "w_up", "w_down")
SHAPES = {"w_gate": (LAYERS, D, FF), "w_up": (LAYERS, D, FF), "w_down": (LAYERS, FF, D)}


def bump(key, n, height):
    away = (jnp.arange(n, dtype=jnp.int32) - jax.random.randint(key, (), 0, n, jnp.int32)) % n
    return jnp.where(away < n // 8, height, 1.0)


def together(key, own, strength):
    shared = jax.random.normal(key, own.shape[1:], jnp.float32)
    return (own + strength * shared) * lax.rsqrt(1 + strength * strength)


def setup_inputs(seed: int = 0, part: int = 0) -> dict:
    kx, kdy, ka, kb, kz, kf, kh, kl, *keys = jax.random.split(jax.random.key(seed), 8 + 3 * len(NAMES))
    kx, kdy, ka, kb = (jax.random.fold_in(k, part) for k in (kx, kdy, ka, kb))
    kw, km, kv = (keys[i::3] for i in range(3))
    shape = (SEQUENCES, TOKENS, D)
    much_x, much_dy = jax.random.uniform(kz, (2,), jnp.float32, 0.0, 1.0)
    loud = 2.0 ** jax.random.uniform(jax.random.fold_in(kz, 1), (), jnp.float32, -1.0, 2.0)
    layers = 2.0 ** jax.random.uniform(kl, (LAYERS, 1, 1), jnp.float32, -1.0, 1.0)
    x = together(ka, jax.random.normal(kx, shape, jnp.float32), much_x) * bump(kf, D, 4.0)
    dy = together(kb, jax.random.normal(kdy, shape, jnp.float32), much_dy)
    drawn = {"x": x.astype(jnp.bfloat16), "dy": (loud * dy * (SEQUENCES * TOKENS) ** -0.5).astype(jnp.bfloat16)}
    for key, name in zip(kw, NAMES, strict=True):
        w = jax.random.normal(key, SHAPES[name], jnp.float32) * SHAPES[name][1] ** -0.5
        drawn[name] = (w * {"w_gate": 1.0, "w_up": bump(kh, FF, 4.0), "w_down": layers}[name]).astype(jnp.bfloat16)
    for key, name in zip(km, NAMES, strict=True):
        drawn[f"m_{name}"] = 0.1 * jax.random.normal(key, SHAPES[name], jnp.float32)
    for key, name in zip(kv, NAMES, strict=True):
        drawn[f"v_{name}"] = jax.random.uniform(key, SHAPES[name], jnp.float32, 0.005, 0.015)
    return drawn


def matmul(a, w):
    return jnp.dot(a, w, preferred_element_type=jnp.float32).astype(jnp.bfloat16)


def normed(h):
    wide = h.astype(jnp.float32)
    scale = lax.rsqrt(jnp.mean(wide**2, -1, keepdims=True) + 1e-6)
    return (wide * scale).astype(jnp.bfloat16)


def layer(h, w):
    a = normed(h)
    gate = jnp.dot(a, w["w_gate"], preferred_element_type=jnp.float32)
    up = jnp.dot(a, w["w_up"], preferred_element_type=jnp.float32)
    return h + matmul((jax.nn.silu(gate) * up).astype(jnp.bfloat16), w["w_down"])


def adamw(w, m, v, g):
    m = 0.9 * m + 0.1 * g
    v = 0.95 * v + 0.05 * g * g
    step = m * lax.rsqrt(v + 1e-8) + 0.1 * w
    return (w - 0.02 * step).astype(jnp.bfloat16), m, v


def clipped(gradients, sum_of_squares, count):
    factor = jnp.minimum(1.0, 0.5 * lax.rsqrt(sum_of_squares / count + 1e-30))
    return [g * factor for g in gradients]


def stack(weights, h):
    return lax.scan(lambda h, w: (layer(h, w), None), h, weights)[0]


def reference(x, dy, w_gate, w_up, w_down, m_w_gate, m_w_up, m_w_down, v_w_gate, v_w_up, v_w_down):
    weights = dict(zip(NAMES, (w_gate, w_up, w_down), strict=True))

    def take(so_far, sequence):
        h, by_y = sequence
        _, back = jax.vjp(lambda w: stack(w, h), weights)
        return jax.tree.map(lambda total, term: total + term.astype(jnp.float32), so_far, back(by_y)[0]), None

    none_yet = {name: jnp.zeros(w.shape, jnp.float32) for name, w in weights.items()}
    by_weights, _ = lax.scan(take, none_yet, (x, dy))
    gradients = [by_weights[name].astype(jnp.bfloat16).astype(jnp.float32) for name in NAMES]
    gradients = clipped(gradients, sum(jnp.sum(g * g) for g in gradients), sum(g.size for g in gradients))
    new = [
        adamw(w.astype(jnp.float32), m, v, g)
        for w, m, v, g in zip((w_gate, w_up, w_down), (m_w_gate, m_w_up, m_w_down), (v_w_gate, v_w_up, v_w_down), gradients, strict=True)
    ]
    return tuple(one[which] for which in range(3) for one in new)
```

```python
import jax
import jax.numpy as jnp
from jax import lax
from jax.sharding import PartitionSpec as P

NAMES = ("w_gate", "w_up", "w_down")


def matmul(a, w):
    return jnp.dot(a, w, preferred_element_type=jnp.float32).astype(jnp.bfloat16)


def normed(h):
    wide = h.astype(jnp.float32)
    scale = lax.rsqrt(jnp.mean(wide**2, -1, keepdims=True) + 1e-6)
    return (wide * scale).astype(jnp.bfloat16)


def layer(h, w_gate, w_up, w_down):
    a = normed(h)
    gate = jnp.dot(a, w_gate, preferred_element_type=jnp.float32)
    up = jnp.dot(a, w_up, preferred_element_type=jnp.float32)
    return h + matmul((jax.nn.silu(gate) * up).astype(jnp.bfloat16), w_down)


def adamw(w, m, v, g):
    m = 0.9 * m + 0.1 * g
    v = 0.95 * v + 0.05 * g * g
    step = m * lax.rsqrt(v + 1e-8) + 0.1 * w
    return (w - 0.02 * step).astype(jnp.bfloat16), m, v


def stack(weights, h):
    for one in weights:
        h = layer(h, *one)
    return h


def solution(mesh):
    members = mesh.shape["dp"]

    def body(x, dy, *arrays):
        weights, m, v = (arrays[i : i + 3] for i in (0, 3, 6))
        layers = weights[0].shape[0]
        _, back = jax.vjp(lambda w: stack(w, x[0]), [tuple(w[i] for w in weights) for i in range(layers)])
        by_weights = back(dy[0])[0]
        mine = {}
        for i in reversed(range(layers)):
            for k in (2, 0, 1):
                mine[k, i] = lax.psum_scatter(by_weights[i][k], "dp", scatter_dimension=0, tiled=True)
        gradients = [jnp.stack([mine[k, i] for i in range(layers)]).astype(jnp.float32) for k in range(3)]
        total = lax.psum(sum(jnp.sum(g * g) for g in gradients), "dp")
        factor = jnp.minimum(1.0, 0.5 * lax.rsqrt(total / sum(w.size for w in weights) + 1e-30))
        me = lax.axis_index("dp")
        new = []
        for w, m_, v_, g in zip(weights, m, v, gradients, strict=True):
            rows = w.shape[1] // members
            own = lax.dynamic_slice_in_dim(w, me * rows, rows, 1).astype(jnp.float32)
            new.append(adamw(own, m_, v_, g * factor))
        gathered = [lax.all_gather(one[0], "dp", axis=1, tiled=True) for one in new]
        return (*gathered, *(one[1] for one in new), *(one[2] for one in new))

    whole, rows = P(), P(None, "dp")
    tokens = P(("rep", "dp"))
    return jax.shard_map(
        body,
        mesh=mesh,
        in_specs=(tokens, tokens, *[whole] * 3, *[rows] * 6),
        out_specs=(*[P("rep")] * 3, *[P("rep", "dp")] * 6),
        check_vma=False,
    )
```
